32 devices in a mesh: pts: 4 (over y, core), dir: 4 (over z), freq: 2 (over x).
Axes of the slice: x: 2, y: 2, z: 4, core: 2. Of those that a mesh axis runs over, the one named last changes fastest.
Arguments:
- action: float32 [48, 64, 16384], P('freq', 'dir', 'pts'), may hold values from 0.05 to 2
- bathymetry: float32 [16384], P('pts'), may hold values from 20 to 60
- refraction: float32 [48, 16384], P('freq', 'pts'), may hold values from 0.5 to 2
- shifting: float32 [48, 16384], P('freq', 'pts'), may hold values from 0.5 to 2
- heading: float32 [16384], P('pts'), may hold values from -3.140625 to 3.140625
- slope_angle: float32 [16384], P('pts'), may hold values from -3.140625 to 3.140625
- wet_mask: int32 [16384], P('pts'), may hold values 0 or 1
- substeps: int32 [32], P('pts'), may hold values from 1 to 4
Outputs:
- evolved: float32 [48, 64, 16384], P('freq', 'dir', 'pts')
The draws below stay inside these ranges and needn't reach their ends.
All inputs are finite; a program needn't handle non-finite values. Where the reference program divides by a largest or mean magnitude, that divisor is 1e-20 or more. No bound on the sum of `wet_mask` on one device may be relied on, other than what follows from the above.
Results may differ from the reference program's by a relative error of at most 0.00002.
Values sent between devices are 32-bit elements; how exact they have to be, the bound alone decides.
A program may use at most 64 MiB of HBM per device.

```python
import math
import jax
import jax.numpy as jnp
from jax import lax

FREQ = 48
DIR = 64
KMAX = 4
BLK = 512
P_DEV = 4096
PTS = 16384
NBLK = 32
N_PTS = 4


def place_ends(array, own_key, low, high):
    dims = array.shape
    spot = [jax.random.randint(jax.random.fold_in(own_key, axis), (), 0, dims[axis]) for axis in range(len(dims))]
    array = array.at[tuple(spot)].set(low)
    longest = dims.index(max(dims))
    spot[longest] = (spot[longest] + 1) % dims[longest]
    return array.at[tuple(spot)].set(high)


def block_scale(rng, dims, shards, least, high):
    def one(dim, parts):
        draws = jax.random.uniform(jax.random.fold_in(jax.random.fold_in(rng, 6), dim), (parts,), jnp.float32, least / len(shards), high / len(shards))
        return jnp.repeat(jnp.exp(draws), dims[dim] // parts).reshape((-1,) + (1,) * (len(dims) - dim - 1))

    gain = one(*shards[0])
    for cut in shards[1:]:
        gain = gain * one(*cut)
    return gain


def setup_inputs(seed: int = 0) -> dict:
    streams_of = jax.random.split(jax.random.key(seed), 9)
    action = jnp.clip(jnp.exp(math.log(2.0) - 3.6888794 * jax.random.uniform(streams_of[0], (FREQ, DIR, PTS), jnp.float32) ** block_scale(streams_of[0], (FREQ, DIR, PTS), ((0, 2), (1, 4), (2, 4)), -0.2, 0.2)), 0.05, 2.0)
    bathymetry = jnp.clip(20.0 + 40.0 * jax.random.uniform(streams_of[1], (PTS,), jnp.float32) ** block_scale(streams_of[1], (PTS,), ((0, 4),), -0.2, 0.2), 20.0, 60.0)
    refraction = jnp.clip(jnp.exp(math.log(2.0) - 1.3862944 * jax.random.uniform(streams_of[2], (FREQ, PTS), jnp.float32) ** block_scale(streams_of[2], (FREQ, PTS), ((0, 2), (1, 4)), -0.2, 0.2)), 0.5, 2.0)
    shifting = jnp.clip(jnp.exp(math.log(2.0) - 1.3862944 * jax.random.uniform(streams_of[3], (FREQ, PTS), jnp.float32) ** block_scale(streams_of[3], (FREQ, PTS), ((0, 2), (1, 4)), -0.2, 0.2)), 0.5, 2.0)
    heading = jnp.clip(jax.random.uniform(streams_of[4], (PTS,), jnp.float32, -3.140625, 3.140625), -3.140625, 3.140625)
    slope_angle = jnp.clip(jax.random.uniform(streams_of[5], (PTS,), jnp.float32, -3.140625, 3.140625), -3.140625, 3.140625)
    wet_mask = place_ends((jax.random.randint(streams_of[6], (PTS,), 0, 4) < 3).astype(jnp.int32), jax.random.fold_in(streams_of[6], 1), 0, 1)
    substeps = place_ends(jax.random.randint(streams_of[7], (NBLK,), 1, KMAX + 1), jax.random.fold_in(streams_of[7], 1), 1, KMAX).astype(jnp.int32)
    return dict(action=action, bathymetry=bathymetry, refraction=refraction, shifting=shifting, heading=heading, slope_angle=slope_angle, wet_mask=wet_mask, substeps=substeps)


EPSILON = 1e-6


def sweep(values, courant, weight, active, along):
    extent = values.shape[along]
    lower_cells = lax.slice_in_dim(values, 0, extent - 1, axis=along)
    upper_cells = lax.slice_in_dim(values, 1, extent, axis=along)
    interface = 0.5 * (lax.slice_in_dim(courant, 0, extent - 1, axis=along) + lax.slice_in_dim(courant, 1, extent, axis=along)) * weight
    fluxes = jnp.maximum(interface, 0.0) * lower_cells + jnp.minimum(interface, 0.0) * upper_cells
    change = lax.slice_in_dim(fluxes, 1, extent - 1, axis=along) - lax.slice_in_dim(fluxes, 0, extent - 2, axis=along)
    inner_cells = lax.slice_in_dim(values, 1, extent - 1, axis=along)
    return jnp.where(active, inner_cells - change, inner_cells)


def direction_angles(index):
    return (index.astype(jnp.float32) + 0.5) * (2.0 * math.pi / DIR)


def reference(action, bathymetry, refraction, shifting, heading, slope_angle, wet_mask, substeps):
    padded = jnp.concatenate([bathymetry[:1], bathymetry, bathymetry[-1:]])
    gradient = (padded[2:] - padded[:-2]) * 0.5
    wet_float = wet_mask.astype(jnp.float32)
    turn_base = refraction * gradient[None, :] * wet_float[None, :]
    shift_base = shifting * wet_float[None, :]
    angles = direction_angles(jnp.arange(DIR, dtype=jnp.int32))
    cos_peak = jnp.max(jnp.abs(jnp.cos(angles[:, None] - heading[None, :])), axis=0)
    sin_peak = jnp.max(jnp.abs(jnp.sin(angles[:, None] - slope_angle[None, :])), axis=0)
    peak_turn = jnp.max(jnp.abs(turn_base) * sin_peak[None, :])
    peak_shift = jnp.max(jnp.abs(shift_base) * cos_peak[None, :])
    scale_turn = 0.5 / (peak_turn + EPSILON)
    scale_shift = 0.5 / (peak_shift + EPSILON)
    point_counts = jnp.repeat(substeps, BLK)
    marks = jnp.arange(FREQ + 1, dtype=jnp.int32)
    freq_weight = jnp.where((marks >= 1) & (marks <= FREQ - 1), 1.0, 0.0).astype(jnp.float32)[:, None, None]

    def one_group(group_index, output):
        start = (group_index * P_DEV).astype(jnp.int32)
        spectrum = lax.dynamic_slice_in_dim(action, start, P_DEV, 2)
        turn_part = lax.dynamic_slice_in_dim(turn_base, start, P_DEV, 1)
        shift_part = lax.dynamic_slice_in_dim(shift_base, start, P_DEV, 1)
        heading_part = lax.dynamic_slice_in_dim(heading, start, P_DEV, 0)
        slope_part = lax.dynamic_slice_in_dim(slope_angle, start, P_DEV, 0)
        wet_part = lax.dynamic_slice_in_dim(wet_float, start, P_DEV, 0)
        count_part = lax.dynamic_slice_in_dim(point_counts, start, P_DEV, 0)
        count_float = count_part.astype(jnp.float32)
        sines = jnp.sin(angles[:, None] - slope_part[None, :])
        c_turn = turn_part[:, None, :] * sines[None, :, :]
        courant_turn = c_turn * scale_turn / count_float[None, None, :]
        courant_wrap = jnp.concatenate([courant_turn[:, -1:], courant_turn, courant_turn[:, :1]], axis=1)
        for sweep_index in range(KMAX):
            active = (sweep_index < count_part)[None, None, :]
            wrapped = jnp.concatenate([spectrum[:, -1:], spectrum, spectrum[:, :1]], axis=1)
            spectrum = sweep(wrapped, courant_wrap, 1.0, active, 1)
        cosines = jnp.cos(angles[:, None] - heading_part[None, :])
        c_shift = shift_part[:, None, :] * cosines[None, :, :]
        courant_shift = c_shift * scale_shift / count_float[None, None, :]
        courant_chain = jnp.pad(courant_shift, ((1, 1), (0, 0), (0, 0)))
        for sweep_index in range(KMAX):
            active = (sweep_index < count_part)[None, None, :]
            chained = jnp.pad(spectrum, ((1, 1), (0, 0), (0, 0)))
            spectrum = sweep(chained, courant_chain, freq_weight, active, 0)
        return lax.dynamic_update_slice_in_dim(output, spectrum * wet_part[None, None, :], start, 2)

    return lax.fori_loop(0, N_PTS, one_group, jnp.zeros_like(action))
```

```python
import functools
import math

import jax
import jax.numpy as jnp
from jax import lax
from jax.experimental import pallas as pl
from jax.experimental.pallas import tpu as pltpu
from jax.sharding import PartitionSpec as P

FREQ = 48
DIR = 64
KMAX = 4
BLK = 512
CHUNK = 256
HALO = KMAX
SUB = 8

EPSILON = 1e-06
MESH = pl.DeviceIdType.MESH


def kernel(
    n_pts,
    n_dir,
    n_freq,
    action_ref,
    head_ref,
    tail_ref,
    depth_ref,
    refraction_ref,
    shifting_ref,
    heading_ref,
    slope_ref,
    wet_ref,
    count_ref,
    out_ref,
    own,
    upper,
    lower,
    ext,
    shext,
    face_shift,
    turn_row,
    shift_row,
    trig,
    depth_in,
    peaks,
    own_sem,
    dir_send,
    dir_recv,
    freq_send,
    freq_recv,
    sh_send,
    sh_recv,
    depth_send,
    depth_recv,
    peak_send,
    peak_recv,
):
    freq_local, dir_local, points = own.shape
    chunks = points // CHUNK
    rows = -(-(dir_local + 2 * HALO) // SUB) * SUB
    pts_at = lax.axis_index("pts")
    dir_at = lax.axis_index("dir")
    freq_at = lax.axis_index("freq")
    dir_up, dir_down = lax.rem(dir_at + 1, n_dir), lax.rem(dir_at + n_dir - 1, n_dir)
    pts_up, pts_down = lax.rem(pts_at + 1, n_pts), lax.rem(pts_at + n_pts - 1, n_pts)
    group = n_pts * n_freq
    member = pts_at * n_freq + freq_at
    has_above = freq_at < n_freq - 1
    has_below = freq_at > 0

    def peer(offset):
        other = lax.rem(member + offset, group)
        return {"pts": other // n_freq, "freq": lax.rem(other, n_freq)}

    barrier = pltpu.get_barrier_semaphore()
    for target in (dir_up, dir_down):
        pl.semaphore_signal(barrier, inc=1, device_id={"dir": target}, device_id_type=MESH)
    for offset in range(1, group):
        pl.semaphore_signal(barrier, inc=1, device_id=peer(offset), device_id_type=MESH)
    pl.semaphore_wait(barrier, 2 + group - 1)

    def span(c):
        return pl.ds(pl.multiple_of(c * CHUNK, CHUNK), CHUNK)

    def remote(src, dst, send, recv, where):
        return pltpu.make_async_remote_copy(
            src_ref=src, dst_ref=dst, send_sem=send, recv_sem=recv, device_id=where, device_id_type=MESH
        )

    def depth_copies():
        return (
            remote(
                depth_ref.at[:, pl.ds(points - 128, 128)],
                depth_in.at[0],
                depth_send.at[0],
                depth_recv.at[0],
                {"pts": pts_up},
            ),
            remote(
                depth_ref.at[:, pl.ds(0, 128)],
                depth_in.at[1],
                depth_send.at[1],
                depth_recv.at[1],
                {"pts": pts_down},
            ),
        )

    def dir_copies(c):
        return (
            remote(
                tail_ref.at[:, :, span(c)],
                lower.at[:, :, span(c)],
                dir_send.at[0, c],
                dir_recv.at[0, c],
                {"dir": dir_up},
            ),
            remote(
                head_ref.at[:, :, span(c)],
                upper.at[:, :, span(c)],
                dir_send.at[1, c],
                dir_recv.at[1, c],
                {"dir": dir_down},
            ),
        )

    def own_copy(c):
        return pltpu.make_async_copy(action_ref.at[:, :, span(c)], own.at[:, :, span(c)], own_sem.at[c])

    above, below = lax.rem(freq_at + 1, n_freq), lax.rem(freq_at + n_freq - 1, n_freq)

    def rise(src, dst, send, recv):
        return remote(src, dst, send, recv, {"freq": above})

    def fall(src, dst, send, recv):
        return remote(src, dst, send, recv, {"freq": below})

    def freq_copies(c):
        return (
            rise(
                ext.at[pl.ds(freq_local, HALO), :, span(c)],
                ext.at[pl.ds(0, HALO), :, span(c)],
                freq_send.at[0, c],
                freq_recv.at[0, c],
            ),
            fall(
                ext.at[pl.ds(HALO, HALO), :, span(c)],
                ext.at[pl.ds(freq_local + HALO, HALO), :, span(c)],
                freq_send.at[1, c],
                freq_recv.at[1, c],
            ),
        )

    def sh_copies():
        return (
            rise(
                shifting_ref.at[pl.ds(freq_local - SUB, SUB)],
                shext.at[0],
                sh_send.at[0],
                sh_recv.at[0],
            ),
            fall(shifting_ref.at[pl.ds(0, SUB)], shext.at[1], sh_send.at[1], sh_recv.at[1]),
        )

    def start_pair(pair):
        @pl.when(has_above)
        def _():
            pair[0].start()

        @pl.when(has_below)
        def _():
            pair[1].start()

    def wait_pair(pair):
        @pl.when(has_above)
        def _():
            pair[0].wait_send()
            pair[1].wait_recv()

        @pl.when(has_below)
        def _():
            pair[1].wait_send()
            pair[0].wait_recv()

    for copy in depth_copies():
        copy.start()

    @pl.loop(0, chunks)
    def _(c):
        for copy in dir_copies(c):
            copy.start()
        own_copy(c).start()

    start_pair(sh_copies())

    row = lax.broadcasted_iota(jnp.int32, (rows, CHUNK), 0)
    offset = jnp.where(row >= rows - HALO, row - rows, row)
    angle = ((dir_at * dir_local + offset).astype(jnp.float32) + 0.5) * (2.0 * math.pi / DIR)
    trig[0] = jnp.sin(angle)
    trig[1] = jnp.cos(angle)
    half = lax.broadcasted_iota(jnp.int32, (DIR // 2, 128), 0)
    half_angle = (half.astype(jnp.float32) + 0.5) * (2.0 * math.pi / DIR)
    half_sin, half_cos = jnp.sin(half_angle), jnp.cos(half_angle)
    wet = wet_ref[...].astype(jnp.float32)
    trig_row = (jnp.sin(slope_ref[...]), jnp.cos(slope_ref[...]), jnp.sin(heading_ref[...]), jnp.cos(heading_ref[...]))
    turn_row[1:2, :] = trig_row[0]
    turn_row[2:3, :] = trig_row[1]
    shift_row[1:2, :] = trig_row[2]
    shift_row[2:3, :] = trig_row[3]

    @pl.when(jnp.logical_not(has_below))
    def _():
        @pl.loop(0, HALO)
        def _(f):
            ext[f] = jnp.zeros((dir_local, points), jnp.float32)

    @pl.when(jnp.logical_not(has_above))
    def _():
        @pl.loop(freq_local + HALO, freq_local + 2 * HALO)
        def _(f):
            ext[f] = jnp.zeros((dir_local, points), jnp.float32)

    for copy in depth_copies():
        copy.wait()
    depth = depth_ref[...]
    lane = lax.broadcasted_iota(jnp.int32, (1, points), 1)
    before = jnp.where(pts_at == 0, depth[:, :1], depth_in[0][:, 127:128])
    after = jnp.where(pts_at == n_pts - 1, depth[:, points - 1 :], depth_in[1][:, :1])
    left = jnp.where(lane == 0, before, pltpu.roll(depth, 1, 1))
    right = jnp.where(lane == points - 1, after, pltpu.roll(depth, points - 1, 1))
    slope = (right - left) * 0.5 * wet
    turn_row[0:1, :] = slope
    shift_row[0:1, :] = wet

    def peak_step(i, carry):
        turn, shift = carry
        part = pl.ds(pl.multiple_of(i * 128, 128), 128)
        sines = jnp.abs(half_sin * turn_row[2:3, part] - half_cos * turn_row[1:2, part])
        cosines = jnp.abs(half_cos * shift_row[2:3, part] + half_sin * shift_row[1:2, part])
        turn_peak = jnp.max(sines, axis=0, keepdims=True) * jnp.abs(turn_row[0:1, part])
        shift_peak = jnp.max(cosines, axis=0, keepdims=True) * shift_row[0:1, part]
        turn = jnp.maximum(turn, jnp.abs(refraction_ref[:, part]) * turn_peak)
        shift = jnp.maximum(shift, jnp.abs(shifting_ref[:, part]) * shift_peak)
        return turn, shift

    zero = jnp.zeros((freq_local, 128), jnp.float32)
    turn, shift = lax.fori_loop(0, points // 128, peak_step, (zero, zero))
    turn = jnp.max(jnp.max(turn, axis=0, keepdims=True), axis=1, keepdims=True)
    shift = jnp.max(jnp.max(shift, axis=0, keepdims=True), axis=1, keepdims=True)
    tile = lax.broadcasted_iota(jnp.int32, (SUB, 128), 0)
    peaks[member] = jnp.where(tile < SUB // 2, turn, shift)

    wait_pair(sh_copies())
    face_rows = freq_local + 2 * HALO
    first = freq_at * freq_local - HALO

    @pl.loop(0, points // CHUNK)
    def _(c):
        part = span(c)
        window = jnp.concatenate(
            [shext[0, :, part][SUB - HALO :], shifting_ref[:, part], shext[1, :, part][:HALO]], axis=0
        )
        following = jnp.concatenate([window[1:], window[:1]], axis=0)
        mark = first + lax.broadcasted_iota(jnp.int32, (face_rows, CHUNK), 0)
        valid = (mark >= 0) & (mark + 1 <= FREQ - 1)
        face_shift[:, part] = jnp.where(valid, 0.5 * (window + following), 0.0)

    def peak_copy(offset):
        return remote(
            peaks.at[member], peaks.at[member], peak_send.at[offset], peak_recv.at[offset], peer(offset)
        )

    def peak_arrival(offset):
        source = lax.rem(member + group - offset, group)
        return remote(
            peaks.at[source], peaks.at[source], peak_send.at[offset], peak_recv.at[offset], peer(offset)
        )

    for offset in range(1, group):
        peak_copy(offset).start()
    for offset in range(1, group):
        peak_copy(offset).wait_send()
        peak_arrival(offset).wait_recv()
    top = jnp.max(peaks[...], axis=0)
    scale_turn = 0.5 / (top[0:1, 0:1] + EPSILON)
    scale_shift = 0.5 / (top[SUB // 2 : SUB // 2 + 1, 0:1] + EPSILON)
    count = count_ref[...].astype(jnp.float32)
    turn_row[0:1, :] = turn_row[0:1, :] * scale_turn / count
    shift_row[3:4, :] = shift_row[0:1, :] * scale_shift / count

    def masks(c):
        per_point = count_ref[:, span(c)]
        return [None] + [jnp.where(per_point > k, 1.0, 0.0) for k in range(1, KMAX)]

    def turn_chunk(c):
        part = span(c)
        for copy in dir_copies(c):
            copy.wait()
        own_copy(c).wait()
        speed = (trig[0] * turn_row[2:3, part] - trig[1] * turn_row[1:2, part]) * turn_row[0:1, part]
        face = 0.5 * (speed + pltpu.roll(speed, rows - 1, 0))
        down = jnp.maximum(face, 0.0)
        up = jnp.minimum(face, 0.0)
        active = masks(c)

        def one(f):
            pieces = [own[f, :, part], upper[f, :, part]]
            spare = rows - dir_local - 2 * HALO
            if spare:
                pieces.append(jnp.zeros((spare, CHUNK), jnp.float32))
            pieces.append(lower[f, :, part])
            cells = jnp.concatenate(pieces, axis=0)
            rate = refraction_ref[pl.ds(f, 1), part]
            for k in range(KMAX):
                flux = down * cells + up * pltpu.roll(cells, rows - 1, 0)
                step = rate if k == 0 else rate * active[k]
                cells = cells - step * (flux - pltpu.roll(flux, 1, 0))
            ext[HALO + f, :, part] = cells[:dir_local]

        for f in range(HALO):
            one(f)
            one(freq_local - HALO + f)

        @pl.loop(HALO, freq_local - HALO, step=2)
        def _(f):
            one(f)
            one(f + 1)

        start_pair(freq_copies(c))

    def shift_chunk(c):
        part = span(c)
        wait_pair(freq_copies(c))
        speed = (
            trig[1, :dir_local] * shift_row[2:3, part] + trig[0, :dir_local] * shift_row[1:2, part]
        ) * shift_row[3:4, part]
        high = jnp.maximum(speed, 0.0)
        low = jnp.minimum(speed, 0.0)
        active = masks(c)
        wet_part = shift_row[0:1, part]
        for k in range(KMAX):
            high_k = high if k == 0 else high * active[k]
            low_k = low if k == 0 else low * active[k]

            def flux_at(j, here, there):
                return face_shift[pl.ds(j, 1), part] * (high_k * here + low_k * there)

            here = ext[k + 1, :, part]
            flux = flux_at(k, ext[k, :, part], here)

            def step(j, carry):
                here, flux = carry
                there = ext[j + 1, :, part]
                beyond = flux_at(j, here, there)
                cells = here - (beyond - flux)
                if k == KMAX - 1:
                    out_ref[j - HALO, :, part] = cells * wet_part
                else:
                    ext[j, :, part] = cells
                return there, beyond

            lax.fori_loop(k + 1, freq_local + 2 * HALO - 1 - k, step, (here, flux), unroll=2)

    turn_chunk(0)

    @pl.loop(1, chunks)
    def _(c):
        turn_chunk(c)
        shift_chunk(c - 1)

    shift_chunk(chunks - 1)


def local(mesh, action, bathymetry, refraction, shifting, heading, slope_angle, wet_mask, substeps):
    freq_local, dir_local, points = action.shape
    n_pts, n_dir, n_freq = mesh.shape["pts"], mesh.shape["dir"], mesh.shape["freq"]
    chunks = points // CHUNK
    rows = -(-(dir_local + 2 * HALO) // SUB) * SUB
    group = n_pts * n_freq
    counts = jnp.broadcast_to(substeps[:, None], (substeps.shape[0], BLK)).reshape(1, points)
    vmem = pl.BlockSpec(memory_space=pltpu.VMEM)
    dma = pltpu.SemaphoreType.DMA
    return pl.pallas_call(
        functools.partial(kernel, n_pts, n_dir, n_freq),
        out_shape=jax.ShapeDtypeStruct(action.shape, jnp.float32),
        in_specs=[pl.BlockSpec(memory_space=pl.ANY)] + [vmem] * 9,
        out_specs=vmem,
        scratch_shapes=[
            pltpu.VMEM((freq_local, dir_local, points), jnp.float32),
            pltpu.VMEM((freq_local, HALO, points), jnp.float32),
            pltpu.VMEM((freq_local, HALO, points), jnp.float32),
            pltpu.VMEM((freq_local + 2 * HALO, dir_local, points), jnp.float32),
            pltpu.VMEM((2, SUB, points), jnp.float32),
            pltpu.VMEM((freq_local + 2 * HALO, points), jnp.float32),
            pltpu.VMEM((SUB, points), jnp.float32),
            pltpu.VMEM((SUB, points), jnp.float32),
            pltpu.VMEM((2, rows, CHUNK), jnp.float32),
            pltpu.VMEM((2, 1, 128), jnp.float32),
            pltpu.VMEM((group, SUB, 128), jnp.float32),
            dma((chunks,)),
            dma((2, chunks)),
            dma((2, chunks)),
            dma((2, chunks)),
            dma((2, chunks)),
            dma((2,)),
            dma((2,)),
            dma((2,)),
            dma((2,)),
            dma((group,)),
            dma((group,)),
        ],
        compiler_params=pltpu.CompilerParams(
            collective_id=0, has_side_effects=True, vmem_limit_bytes=60 * 1024 * 1024
        ),
    )(
        action,
        lax.slice_in_dim(action, 0, HALO, axis=1),
        lax.slice_in_dim(action, dir_local - HALO, dir_local, axis=1),
        bathymetry.reshape(1, points),
        refraction,
        shifting,
        heading.reshape(1, points),
        slope_angle.reshape(1, points),
        wet_mask.reshape(1, points),
        counts,
    )


def solution(mesh):
    placed = (
        P("freq", "dir", "pts"),
        P("pts"),
        P("freq", "pts"),
        P("freq", "pts"),
        P("pts"),
        P("pts"),
        P("pts"),
        P("pts"),
    )
    return jax.shard_map(
        functools.partial(local, mesh),
        mesh=mesh,
        in_specs=placed,
        out_specs=P("freq", "dir", "pts"),
        check_vma=False,
    )
```

```python
import functools
import math

import jax
import jax.numpy as jnp
from jax import lax
from jax.experimental import pallas as pl
from jax.experimental.pallas import tpu as pltpu
from jax.sharding import PartitionSpec as P

FREQ = 48
DIR = 64
KMAX = 4
BLK = 512
CHUNK = 256
HALO = KMAX
SUB = 8

EPSILON = 1e-06
MESH = pl.DeviceIdType.MESH


def kernel(
    n_pts,
    n_dir,
    n_freq,
    action_ref,
    depth_ref,
    refraction_ref,
    shifting_ref,
    heading_ref,
    slope_ref,
    wet_ref,
    substeps_ref,
    out_ref,
    own,
    upper,
    lower,
    ext,
    shext,
    face_shift,
    turn_row,
    shift_row,
    count_row,
    trig,
    depth_in,
    peaks,
    own_sem,
    dir_send,
    dir_recv,
    freq_send,
    freq_recv,
    sh_send,
    sh_recv,
    depth_send,
    depth_recv,
    peak_send,
    peak_recv,
):
    freq_local, dir_local, points = own.shape
    chunks = points // CHUNK
    rows = -(-(dir_local + 2 * HALO) // SUB) * SUB
    pts_at = lax.axis_index("pts")
    dir_at = lax.axis_index("dir")
    freq_at = lax.axis_index("freq")
    dir_up, dir_down = lax.rem(dir_at + 1, n_dir), lax.rem(dir_at + n_dir - 1, n_dir)
    pts_up, pts_down = lax.rem(pts_at + 1, n_pts), lax.rem(pts_at + n_pts - 1, n_pts)
    group = n_pts * n_freq
    member = pts_at * n_freq + freq_at
    has_above = freq_at < n_freq - 1
    has_below = freq_at > 0

    def peer(offset):
        other = lax.rem(member + offset, group)
        return {"pts": other // n_freq, "freq": lax.rem(other, n_freq)}

    barrier = pltpu.get_barrier_semaphore()
    for target in (dir_up, dir_down):
        pl.semaphore_signal(barrier, inc=1, device_id={"dir": target}, device_id_type=MESH)
    for offset in range(1, group):
        pl.semaphore_signal(barrier, inc=1, device_id=peer(offset), device_id_type=MESH)
    pl.semaphore_wait(barrier, 2 + group - 1)

    def span(c):
        return pl.ds(pl.multiple_of(c * CHUNK, CHUNK), CHUNK)

    def remote(src, dst, send, recv, where):
        return pltpu.make_async_remote_copy(
            src_ref=src, dst_ref=dst, send_sem=send, recv_sem=recv, device_id=where, device_id_type=MESH
        )

    def depth_copies():
        return (
            remote(
                depth_ref.at[:, pl.ds(points - 128, 128)],
                depth_in.at[0],
                depth_send.at[0],
                depth_recv.at[0],
                {"pts": pts_up},
            ),
            remote(
                depth_ref.at[:, pl.ds(0, 128)],
                depth_in.at[1],
                depth_send.at[1],
                depth_recv.at[1],
                {"pts": pts_down},
            ),
        )

    def dir_copies(c):
        return (
            remote(
                action_ref.at[:, pl.ds(dir_local - HALO, HALO), span(c)],
                lower.at[:, :, span(c)],
                dir_send.at[0, c],
                dir_recv.at[0, c],
                {"dir": dir_up},
            ),
            remote(
                action_ref.at[:, pl.ds(0, HALO), span(c)],
                upper.at[:, :, span(c)],
                dir_send.at[1, c],
                dir_recv.at[1, c],
                {"dir": dir_down},
            ),
        )

    def own_copy(c):
        return pltpu.make_async_copy(action_ref.at[:, :, span(c)], own.at[:, :, span(c)], own_sem.at[c])

    above, below = lax.rem(freq_at + 1, n_freq), lax.rem(freq_at + n_freq - 1, n_freq)

    def rise(src, dst, send, recv):
        return remote(src, dst, send, recv, {"freq": above})

    def fall(src, dst, send, recv):
        return remote(src, dst, send, recv, {"freq": below})

    def freq_copies(c):
        return (
            rise(
                ext.at[pl.ds(freq_local, HALO), :, span(c)],
                ext.at[pl.ds(0, HALO), :, span(c)],
                freq_send.at[0, c],
                freq_recv.at[0, c],
            ),
            fall(
                ext.at[pl.ds(HALO, HALO), :, span(c)],
                ext.at[pl.ds(freq_local + HALO, HALO), :, span(c)],
                freq_send.at[1, c],
                freq_recv.at[1, c],
            ),
        )

    def sh_copies():
        return (
            rise(
                shifting_ref.at[pl.ds(freq_local - SUB, SUB)],
                shext.at[0],
                sh_send.at[0],
                sh_recv.at[0],
            ),
            fall(shifting_ref.at[pl.ds(0, SUB)], shext.at[1], sh_send.at[1], sh_recv.at[1]),
        )

    def start_pair(pair):
        @pl.when(has_above)
        def _():
            pair[0].start()

        @pl.when(has_below)
        def _():
            pair[1].start()

    def wait_pair(pair):
        @pl.when(has_above)
        def _():
            pair[0].wait_send()
            pair[1].wait_recv()

        @pl.when(has_below)
        def _():
            pair[1].wait_send()
            pair[0].wait_recv()

    for copy in depth_copies():
        copy.start()

    @pl.loop(0, chunks)
    def _(c):
        for copy in dir_copies(c):
            copy.start()
        own_copy(c).start()

    start_pair(sh_copies())

    row = lax.broadcasted_iota(jnp.int32, (rows, CHUNK), 0)
    offset = jnp.where(row >= rows - HALO, row - rows, row)
    angle = ((dir_at * dir_local + offset).astype(jnp.float32) + 0.5) * (2.0 * math.pi / DIR)
    trig[0] = jnp.sin(angle)
    trig[1] = jnp.cos(angle)
    half = lax.broadcasted_iota(jnp.int32, (DIR // 2, 128), 0)
    half_angle = (half.astype(jnp.float32) + 0.5) * (2.0 * math.pi / DIR)
    half_sin, half_cos = jnp.sin(half_angle), jnp.cos(half_angle)
    wet = wet_ref[...].astype(jnp.float32)
    trig_row = (jnp.sin(slope_ref[...]), jnp.cos(slope_ref[...]), jnp.sin(heading_ref[...]), jnp.cos(heading_ref[...]))
    turn_row[1:2, :] = trig_row[0]
    turn_row[2:3, :] = trig_row[1]
    shift_row[1:2, :] = trig_row[2]
    shift_row[2:3, :] = trig_row[3]

    @pl.when(jnp.logical_not(has_below))
    def _():
        @pl.loop(0, HALO)
        def _(f):
            ext[f] = jnp.zeros((dir_local, points), jnp.float32)

    @pl.when(jnp.logical_not(has_above))
    def _():
        @pl.loop(freq_local + HALO, freq_local + 2 * HALO)
        def _(f):
            ext[f] = jnp.zeros((dir_local, points), jnp.float32)

    for copy in depth_copies():
        copy.wait()
    depth = depth_ref[...]
    lane = lax.broadcasted_iota(jnp.int32, (1, points), 1)
    before = jnp.where(pts_at == 0, depth[:, :1], depth_in[0][:, 127:128])
    after = jnp.where(pts_at == n_pts - 1, depth[:, points - 1 :], depth_in[1][:, :1])
    left = jnp.where(lane == 0, before, pltpu.roll(depth, 1, 1))
    right = jnp.where(lane == points - 1, after, pltpu.roll(depth, points - 1, 1))
    slope = (right - left) * 0.5 * wet
    turn_row[0:1, :] = slope
    shift_row[0:1, :] = wet

    def peak_step(i, carry):
        turn, shift = carry
        part = pl.ds(pl.multiple_of(i * 128, 128), 128)
        sines = jnp.abs(half_sin * turn_row[2:3, part] - half_cos * turn_row[1:2, part])
        cosines = jnp.abs(half_cos * shift_row[2:3, part] + half_sin * shift_row[1:2, part])
        turn_peak = jnp.max(sines, axis=0, keepdims=True) * jnp.abs(turn_row[0:1, part])
        shift_peak = jnp.max(cosines, axis=0, keepdims=True) * shift_row[0:1, part]
        turn = jnp.maximum(turn, jnp.abs(refraction_ref[:, part]) * turn_peak)
        shift = jnp.maximum(shift, jnp.abs(shifting_ref[:, part]) * shift_peak)
        return turn, shift

    zero = jnp.zeros((freq_local, 128), jnp.float32)
    turn, shift = lax.fori_loop(0, points // 128, peak_step, (zero, zero))
    turn = jnp.max(jnp.max(turn, axis=0, keepdims=True), axis=1, keepdims=True)
    shift = jnp.max(jnp.max(shift, axis=0, keepdims=True), axis=1, keepdims=True)
    tile = lax.broadcasted_iota(jnp.int32, (SUB, 128), 0)
    peaks[member] = jnp.where(tile < SUB // 2, turn, shift)

    wait_pair(sh_copies())
    face_rows = freq_local + 2 * HALO
    first = freq_at * freq_local - HALO

    @pl.loop(0, points // CHUNK)
    def _(c):
        part = span(c)
        window = jnp.concatenate(
            [shext[0, :, part][SUB - HALO :], shifting_ref[:, part], shext[1, :, part][:HALO]], axis=0
        )
        following = jnp.concatenate([window[1:], window[:1]], axis=0)
        mark = first + lax.broadcasted_iota(jnp.int32, (face_rows, CHUNK), 0)
        valid = (mark >= 0) & (mark + 1 <= FREQ - 1)
        face_shift[:, part] = jnp.where(valid, 0.5 * (window + following), 0.0)

    def peak_copy(offset):
        return remote(
            peaks.at[member], peaks.at[member], peak_send.at[offset], peak_recv.at[offset], peer(offset)
        )

    def peak_arrival(offset):
        source = lax.rem(member + group - offset, group)
        return remote(
            peaks.at[source], peaks.at[source], peak_send.at[offset], peak_recv.at[offset], peer(offset)
        )

    for offset in range(1, group):
        peak_copy(offset).start()
    for offset in range(1, group):
        peak_copy(offset).wait_send()
        peak_arrival(offset).wait_recv()
    top = jnp.max(peaks[...], axis=0)
    scale_turn = 0.5 / (top[0:1, 0:1] + EPSILON)
    scale_shift = 0.5 / (top[SUB // 2 : SUB // 2 + 1, 0:1] + EPSILON)
    for block in range(points // BLK):
        part = pl.ds(block * BLK, BLK)
        count_row[0:1, part] = jnp.broadcast_to(
            substeps_ref[0:1, block : block + 1].astype(jnp.float32), (1, BLK)
        )
    count = count_row[0:1, :]
    turn_row[0:1, :] = turn_row[0:1, :] * scale_turn / count
    shift_row[3:4, :] = shift_row[0:1, :] * scale_shift / count

    def masks(c):
        per_point = count_row[0:1, span(c)]
        return [None] + [jnp.where(per_point > k, 1.0, 0.0) for k in range(1, KMAX)]

    def turn_chunk(c):
        part = span(c)
        for copy in dir_copies(c):
            copy.wait()
        own_copy(c).wait()
        speed = (trig[0] * turn_row[2:3, part] - trig[1] * turn_row[1:2, part]) * turn_row[0:1, part]
        face = 0.5 * (speed + pltpu.roll(speed, rows - 1, 0))
        down = jnp.maximum(face, 0.0)
        up = jnp.minimum(face, 0.0)
        active = masks(c)

        def one(f):
            pieces = [own[f, :, part], upper[f, :, part]]
            spare = rows - dir_local - 2 * HALO
            if spare:
                pieces.append(jnp.zeros((spare, CHUNK), jnp.float32))
            pieces.append(lower[f, :, part])
            cells = jnp.concatenate(pieces, axis=0)
            rate = refraction_ref[pl.ds(f, 1), part]
            for k in range(KMAX):
                flux = down * cells + up * pltpu.roll(cells, rows - 1, 0)
                step = rate if k == 0 else rate * active[k]
                cells = cells - step * (flux - pltpu.roll(flux, 1, 0))
            ext[HALO + f, :, part] = cells[:dir_local]

        for f in range(HALO):
            one(f)
            one(freq_local - HALO + f)

        @pl.loop(HALO, freq_local - HALO, step=2)
        def _(f):
            one(f)
            one(f + 1)

        start_pair(freq_copies(c))

    def shift_chunk(c):
        part = span(c)
        wait_pair(freq_copies(c))
        speed = (
            trig[1, :dir_local] * shift_row[2:3, part] + trig[0, :dir_local] * shift_row[1:2, part]
        ) * shift_row[3:4, part]
        high = jnp.maximum(speed, 0.0)
        low = jnp.minimum(speed, 0.0)
        active = masks(c)
        wet_part = shift_row[0:1, part]
        for k in range(KMAX):
            high_k = high if k == 0 else high * active[k]
            low_k = low if k == 0 else low * active[k]

            def flux_at(j, here, there):
                return face_shift[pl.ds(j, 1), part] * (high_k * here + low_k * there)

            here = ext[k + 1, :, part]
            flux = flux_at(k, ext[k, :, part], here)

            def step(j, carry):
                here, flux = carry
                there = ext[j + 1, :, part]
                beyond = flux_at(j, here, there)
                cells = here - (beyond - flux)
                if k == KMAX - 1:
                    out_ref[j - HALO, :, part] = cells * wet_part
                else:
                    ext[j, :, part] = cells
                return there, beyond

            lax.fori_loop(k + 1, freq_local + 2 * HALO - 1 - k, step, (here, flux), unroll=2)

    turn_chunk(0)

    @pl.loop(1, chunks)
    def _(c):
        turn_chunk(c)
        shift_chunk(c - 1)

    shift_chunk(chunks - 1)


def local(mesh, action, bathymetry, refraction, shifting, heading, slope_angle, wet_mask, substeps):
    freq_local, dir_local, points = action.shape
    n_pts, n_dir, n_freq = mesh.shape["pts"], mesh.shape["dir"], mesh.shape["freq"]
    chunks = points // CHUNK
    rows = -(-(dir_local + 2 * HALO) // SUB) * SUB
    group = n_pts * n_freq
    vmem = pl.BlockSpec(memory_space=pltpu.VMEM)
    dma = pltpu.SemaphoreType.DMA
    return pl.pallas_call(
        functools.partial(kernel, n_pts, n_dir, n_freq),
        out_shape=jax.ShapeDtypeStruct(action.shape, jnp.float32),
        in_specs=[pl.BlockSpec(memory_space=pltpu.HBM)] + [vmem] * 7,
        out_specs=vmem,
        scratch_shapes=[
            pltpu.VMEM((freq_local, dir_local, points), jnp.float32),
            pltpu.VMEM((freq_local, HALO, points), jnp.float32),
            pltpu.VMEM((freq_local, HALO, points), jnp.float32),
            pltpu.VMEM((freq_local + 2 * HALO, dir_local, points), jnp.float32),
            pltpu.VMEM((2, SUB, points), jnp.float32),
            pltpu.VMEM((freq_local + 2 * HALO, points), jnp.float32),
            pltpu.VMEM((SUB, points), jnp.float32),
            pltpu.VMEM((SUB, points), jnp.float32),
            pltpu.VMEM((SUB, points), jnp.float32),
            pltpu.VMEM((2, rows, CHUNK), jnp.float32),
            pltpu.VMEM((2, 1, 128), jnp.float32),
            pltpu.VMEM((group, SUB, 128), jnp.float32),
            dma((chunks,)),
            dma((2, chunks)),
            dma((2, chunks)),
            dma((2, chunks)),
            dma((2, chunks)),
            dma((2,)),
            dma((2,)),
            dma((2,)),
            dma((2,)),
            dma((group,)),
            dma((group,)),
        ],
        compiler_params=pltpu.CompilerParams(
            collective_id=0, has_side_effects=True, vmem_limit_bytes=44 * 1024 * 1024
        ),
    )(
        action,
        bathymetry.reshape(1, points),
        refraction,
        shifting,
        heading.reshape(1, points),
        slope_angle.reshape(1, points),
        wet_mask.reshape(1, points),
        substeps.reshape(1, -1),
    )


def solution(mesh):
    placed = (
        P("freq", "dir", "pts"),
        P("pts"),
        P("freq", "pts"),
        P("freq", "pts"),
        P("pts"),
        P("pts"),
        P("pts"),
        P("pts"),
    )
    return jax.shard_map(
        functools.partial(local, mesh),
        mesh=mesh,
        in_specs=placed,
        out_specs=P("freq", "dir", "pts"),
        check_vma=False,
    )
```
